32 devices in a mesh: batch: 4 (over z), seq: 8 (over y, x, core).
Axes of the slice: x: 2, y: 2, z: 4, core: 2. Of those that a mesh axis runs over, the one named last changes fastest.
Arguments:
- hidden: bfloat16 [4, 4096, 4096], P('batch', 'seq'), may hold values from -6 to 6
- score_direction: bfloat16 [4, 4096, 4096], P('batch', 'seq'), may hold values from -6 to 6
- adapter_down: bfloat16 [4096, 256], replicated, may hold values from -0.09375 to 0.09375
- adapter_up: bfloat16 [4096, 256], replicated, may hold values from -0.09375 to 0.09375
- rewards: float32 [4, 4096], P('batch', 'seq'), may hold values from -0.3125 to 0.3125
- values: float32 [4, 4096], P('batch', 'seq'), may hold values from -120 to 120
- log_ratio: float32 [4, 4096], P('batch', 'seq'), may hold values from -4 to 4
- lengths: int32 [4], P('batch'), may hold values from 1024 to 4096
Outputs:
- returns: float32 [4, 4096], P('batch', 'seq')
- grad_down: float32 [4096, 256], P(('batch', 'seq'))
- grad_up: float32 [4096, 256], P(('batch', 'seq'))
The draws below stay inside these ranges and needn't reach their ends.
All inputs are finite; a program needn't handle non-finite values.
Results may differ from the reference program's by a relative error of at most 0.0029.
Values sent between devices are 32-bit elements; how exact they have to be, the bound alone decides.
No kernel may reach another device: no remote copies, remote signals or barrier semaphores. Data moves between devices by JAX's collectives and lax.ppermute only.
A program may use at most 128 MiB of HBM per device.

```python
import math
import jax
import jax.numpy as jnp
from jax import lax

MODEL_DIM = 4096
ADAPTER_RANK = 256
SEQS = 4
LEN = 4096
N_SEQ = 8


def draw_values(key, part):
    base = jax.random.normal(jax.random.fold_in(key, 11), (SEQS, LEN), jnp.float32)
    base = jnp.clip(base, -6.0, 6.0)
    return base


def place_ends(result, own_key, smallest, top_value):
    longest = result.shape.index(max(result.shape))
    spots = []
    for shift in (0, 1):
        where = [jax.random.randint(jax.random.fold_in(own_key, axis), (), 0, length) for axis, length in enumerate(result.shape)]
        where[longest] = (where[longest] + shift) % result.shape[longest]
        spots.append(tuple(where))
    return result.at[spots[0]].set(smallest).at[spots[1]].set(top_value)


def level_of(own_key, extent, cuts, low, largest):
    level = 1.0
    for dim, parts in cuts:
        heights = jax.random.uniform(jax.random.fold_in(jax.random.fold_in(own_key, 6), dim), (parts,), jnp.float32, low / len(cuts), largest / len(cuts))
        level = level * jnp.repeat(jnp.exp(heights), extent[dim] // parts).reshape((-1,) + (1,) * (len(extent) - 1 - dim))
    return level


def noise(stream_key, shape, width, most, split=(), kind=jnp.bfloat16):
    level = level_of(stream_key, shape, split, -0.22, 0.18) if split else 1.0
    array = jax.random.normal(stream_key, shape, jnp.float32) * width * level
    return jnp.minimum(jnp.maximum(array, -most), most).astype(kind)


def setup_inputs(seed: int = 0) -> dict:
    key_of = jax.random.split(jax.random.key(seed), 9)
    hidden = noise(key_of[0], (SEQS, LEN, MODEL_DIM), 1.0, 6.0, ((0, 4), (1, 8)))
    score_direction = noise(key_of[1], (SEQS, LEN, MODEL_DIM), 1.0, 6.0, ((0, 4), (1, 8)))
    adapter_down = noise(key_of[2], (MODEL_DIM, ADAPTER_RANK), MODEL_DIM ** -0.5, 0.09375)
    adapter_up = noise(key_of[3], (MODEL_DIM, ADAPTER_RANK), MODEL_DIM ** -0.5, 0.09375)
    rewards = noise(key_of[4], (SEQS, LEN), 0.02, 0.3125, ((0, 4), (1, 8)), jnp.float32)
    values = draw_values(jax.random.fold_in(key_of[8], 71), 0)
    log_ratio = noise(key_of[6], (SEQS, LEN), 0.3, 4.0, ((0, 4), (1, 8)), jnp.float32)
    lengths = place_ends(jax.random.randint(key_of[7], (SEQS,), LEN // 4, LEN + 1), jax.random.fold_in(key_of[7], 1), LEN // 4, LEN).astype(jnp.int32)
    return {"hidden": hidden, "score_direction": score_direction, "adapter_down": adapter_down, "adapter_up": adapter_up, "rewards": rewards, "values": values, "log_ratio": log_ratio, "lengths": lengths}


ratio_cap = 2.0
weight_gain = 0.08

def reference(hidden, score_direction, adapter_down, adapter_up, rewards, values, log_ratio, lengths):
    seq_count, total_len, model_width = hidden.shape
    low_rank_product = adapter_down.shape[1]
    shard_len = total_len // N_SEQ
    positions = jnp.arange(total_len, dtype=jnp.int32)
    valid = (positions[None, :] < lengths[:, None]).astype(jnp.float32)
    live = (rewards * valid).reshape(seq_count, N_SEQ, shard_len)
    inner = jnp.arange(shard_len, dtype=jnp.int32)
    offsets = (inner[None, :] - inner[:, None]).astype(jnp.float32)
    discount_mat = jnp.where(offsets >= 0, jnp.exp(-offsets / total_len), jnp.zeros_like(offsets))
    within = jnp.einsum('sbk,tk->sbt', live, discount_mat, precision=lax.Precision.HIGHEST)
    firsts = within[:, :, 0]
    block_decay = jnp.exp(jnp.asarray(-shard_len / total_len, jnp.float32))

    def advance(incoming, first_now):
        return (first_now + block_decay * incoming, incoming)
    zeros_seq = jnp.zeros((seq_count,), jnp.float32)
    _, carried = lax.scan(advance, zeros_seq, jnp.transpose(firsts)[::-1])
    carried = jnp.transpose(carried[::-1])
    tail_decay = jnp.exp(-(shard_len - inner).astype(jnp.float32) / total_len)
    returns = (within + tail_decay[None, None, :] * carried[:, :, None]).reshape(seq_count, total_len)
    advantage = returns - values
    adapter_scale = 1.0 / math.sqrt(low_rank_product)
    seq_weight = weight_gain * math.sqrt(total_len * low_rank_product / seq_count) / lengths.astype(jnp.float32)

    def per_seq(totals, pieces):
        hidden_rows, direction_rows, adv_seq, gap_seq, valid_seq, weight_seq = pieces
        down_projected = jnp.dot(hidden_rows, adapter_down, preferred_element_type=jnp.float32)
        up_projected = jnp.dot(direction_rows, adapter_up, preferred_element_type=jnp.float32)
        weight_update = adapter_scale * lax.optimization_barrier(jnp.sum(down_projected * up_projected, axis=-1))
        importance = jnp.exp(gap_seq + weight_update)
        token_weights = valid_seq * jnp.minimum(importance, ratio_cap) * adv_seq * weight_seq
        up_scaled_map = (-adapter_scale * token_weights[:, None] * up_projected).astype(jnp.bfloat16)
        down_scaled_map = (-adapter_scale * token_weights[:, None] * down_projected).astype(jnp.bfloat16)
        dims = (((0,), (0,)), ((), ()))
        grad_a = lax.dot_general(hidden_rows, up_scaled_map, dims, preferred_element_type=jnp.float32)
        grad_b = lax.dot_general(direction_rows, down_scaled_map, dims, preferred_element_type=jnp.float32)
        return ((totals[0] + grad_a, totals[1] + grad_b), None)
    empty = jnp.zeros((model_width, low_rank_product), jnp.float32)
    (raw_down, raw_up), _ = lax.scan(per_seq, (empty, empty), (hidden, score_direction, advantage, log_ratio, valid, seq_weight))
    grad_norm = jnp.sqrt(jnp.sum(raw_down * raw_down) + jnp.sum(raw_up * raw_up))
    clip_norm = 0.5 * math.sqrt(2.0 * model_width * low_rank_product)
    factor = clip_norm / jnp.maximum(grad_norm, clip_norm)
    return (returns, raw_down * factor, raw_up * factor)
```

```python
import functools
import math

import jax
import jax.numpy as jnp
from jax import lax
from jax.experimental import pallas as pl
from jax.experimental.pallas import tpu as pltpu
from jax.sharding import PartitionSpec as P


ratio_cap = 2.0
weight_gain = 0.08
AXES = ("batch", "seq")
LANES = 128
F32 = jnp.float32


def swap(x, mask, count):
    return lax.ppermute(x, AXES, [(i, i ^ mask) for i in range(count)])


def vmem(n):
    return [pl.BlockSpec(memory_space=pltpu.VMEM)] * n


SMEM = pl.BlockSpec(memory_space=pltpu.SMEM)


def project_body(hid, down, direction, up, live, down_t, up_t, within, *, total_len):
    tokens, width = hid.shape
    rank = down.shape[1]
    step = width // 8
    for src, mat, out in ((hid, down, down_t), (direction, up, up_t)):
        acc = jnp.zeros((tokens, rank), F32)
        for k in range(0, width, step):
            acc = acc + jnp.dot(src[:, k : k + step], mat[k : k + step, :], preferred_element_type=F32)
        out[...] = acc.T
    at_k = lax.broadcasted_iota(jnp.int32, (1, tokens), 1).astype(F32)
    row = live[...] * jnp.exp(-at_k / total_len)
    first = row.astype(jnp.bfloat16)
    rest = row - first.astype(F32)
    second = rest.astype(jnp.bfloat16)
    third = (rest - second.astype(F32)).astype(jnp.bfloat16)
    rows = jnp.concatenate([first, second, third], axis=0)
    k_of = lax.broadcasted_iota(jnp.int32, (tokens, tokens), 0)
    t_of = lax.broadcasted_iota(jnp.int32, (tokens, tokens), 1)
    mask = (k_of >= t_of).astype(jnp.bfloat16)
    sums = jnp.dot(rows, mask, preferred_element_type=F32)
    within[...] = jnp.sum(sums, axis=0, keepdims=True) * jnp.exp(at_k / total_len)


def project(hid, down, direction, up, live, total_len):
    tokens, rank = hid.shape[0], down.shape[1]
    return pl.pallas_call(
        functools.partial(project_body, total_len=float(total_len)),
        out_shape=(
            jax.ShapeDtypeStruct((rank, tokens), F32),
            jax.ShapeDtypeStruct((rank, tokens), F32),
            jax.ShapeDtypeStruct((1, tokens), F32),
        ),
        in_specs=vmem(5),
        out_specs=tuple(vmem(3)),
        name="project",
    )(hid, down, direction, up, live)


def weigh_body(length, down_t, up_t, within, carried, values, log_ratio, returns, scaled_up, scaled_down, *, shards, total_len, seq_total):
    rank, tokens = down_t.shape
    shard = lax.axis_index("seq")
    at = lax.broadcasted_iota(jnp.int32, (1, tokens), 1)
    tail = jnp.exp((at - tokens).astype(F32) / total_len)
    back = within[...] + tail * carried[0:1, 0:1]
    returns[...] = back
    adapter_scale = 1.0 / math.sqrt(rank)
    delta = adapter_scale * jnp.sum(down_t[...] * up_t[...], axis=0, keepdims=True)
    importance = jnp.exp(log_ratio[...] + delta)
    count = length[0]
    lens = jnp.full((1, tokens), count, jnp.int32).astype(F32)
    gain = weight_gain * math.sqrt(total_len * rank / seq_total) / lens
    valid = jnp.where(at + shard * tokens < count, 1.0, 0.0)
    weight = -adapter_scale * (valid * jnp.minimum(importance, ratio_cap) * (back - values[...]) * gain)
    scaled_up[...] = (weight * up_t[...]).astype(jnp.bfloat16)
    scaled_down[...] = (weight * down_t[...]).astype(jnp.bfloat16)


def weigh(length, down_t, up_t, within, carried, values, log_ratio, **sizes):
    rank, tokens = down_t.shape
    return pl.pallas_call(
        functools.partial(weigh_body, **sizes),
        out_shape=(
            jax.ShapeDtypeStruct((1, tokens), F32),
            jax.ShapeDtypeStruct((rank, tokens), jnp.bfloat16),
            jax.ShapeDtypeStruct((rank, tokens), jnp.bfloat16),
        ),
        in_specs=[SMEM] + vmem(6),
        out_specs=tuple(vmem(3)),
        name="weigh",
    )(length, down_t, up_t, within, carried, values, log_ratio)


def blocks_body(*refs, jobs, seq_size, n_out, adds):
    hid, direction, scaled_up, scaled_down = refs[:4]
    received = refs[4 : 4 + n_out] if adds else ()
    outs = refs[4 + n_out :] if adds else refs[4:]
    me = lax.axis_index("batch") * seq_size + lax.axis_index("seq")
    for out_at, tiles, row_at, rows, side, from_row in jobs:
        src, weight = ((hid, scaled_up), (direction, scaled_down))[side]
        out = outs[out_at]
        for i in range(0, len(tiles), 2):
            pair = tiles[i : i + 2]
            cols = [src[:, pl.ds(pl.multiple_of((t ^ me) * LANES, LANES), LANES)] for t in pair]
            block = jnp.concatenate(cols, axis=1) if len(cols) > 1 else cols[0]
            grad = jnp.dot(weight[from_row : from_row + rows, :], block, preferred_element_type=F32)
            for j in range(len(pair)):
                part = grad[:, j * LANES : (j + 1) * LANES]
                if adds:
                    part = part + received[out_at][i + j, row_at : row_at + rows, :]
                out[i + j, row_at : row_at + rows, :] = part


def blocks(ops, wanted, received, seq_size, name):
    jobs, shapes = [], []
    for out_at, (tiles, parts) in enumerate(wanted):
        at = 0
        for side, from_row, rows in parts:
            jobs.append((out_at, tuple(tiles), at, rows, side, from_row))
            at += rows
        shapes.append(jax.ShapeDtypeStruct((len(tiles), at, LANES), F32))
    extra = list(received) if received is not None else []
    return pl.pallas_call(
        functools.partial(
            blocks_body, jobs=tuple(jobs), seq_size=seq_size, n_out=len(wanted), adds=received is not None
        ),
        out_shape=tuple(shapes),
        in_specs=vmem(4 + len(extra)),
        out_specs=tuple(vmem(len(wanted))),
        name=name,
    )(*ops, *extra)


def fold_body(*refs, n):
    keeps, gots, send, keep = refs[:n], refs[n : 2 * n], refs[2 * n], refs[2 * n + 1]
    half = send.shape[0]
    at = 0
    for k, g in zip(keeps, gots):
        rows = k.shape[1]
        for i in range(half):
            send[i, at : at + rows, :] = k[half + i] + g[half + i]
            keep[i, at : at + rows, :] = k[i] + g[i]
        at += rows


def fold(pairs, name):
    n = len(pairs)
    half = pairs[0][0].shape[0] // 2
    rows = sum(k.shape[1] for k, _ in pairs)
    shape = jax.ShapeDtypeStruct((half, rows, LANES), F32)
    return pl.pallas_call(
        functools.partial(fold_body, n=n),
        out_shape=(shape, shape),
        in_specs=vmem(2 * n),
        out_specs=tuple(vmem(2)),
        name=name,
    )(*[k for k, _ in pairs], *[g for _, g in pairs])


def total_body(keep_ab, got_ab, keep_c, got_c, down, up, squares, *, cut, rank):
    ab = keep_ab[0] + got_ab[0]
    c = keep_c[0] + got_c[0]
    down[:cut, :] = ab[:cut]
    down[cut:, :] = c[: rank - cut]
    up[:cut, :] = ab[cut:]
    up[cut:, :] = c[rank - cut :]
    row = jnp.sum(ab * ab, axis=0, keepdims=True) + jnp.sum(c * c, axis=0, keepdims=True)
    squares[...] = jnp.broadcast_to(row[None], squares.shape)


def total(keep_ab, got_ab, keep_c, got_c, cut, rank, count):
    return pl.pallas_call(
        functools.partial(total_body, cut=cut, rank=rank),
        out_shape=(
            jax.ShapeDtypeStruct((rank, LANES), F32),
            jax.ShapeDtypeStruct((rank, LANES), F32),
            jax.ShapeDtypeStruct((count, 1, LANES), F32),
        ),
        in_specs=vmem(4),
        out_specs=tuple(vmem(3)),
        name="total",
    )(keep_ab, got_ab, keep_c, got_c)


def clip_body(down, up, squares, grad_down, grad_up, *, clip_norm):
    norm = jnp.sqrt(jnp.sum(jnp.sum(squares[...], axis=0), axis=1, keepdims=True))
    factor = clip_norm / jnp.maximum(norm, clip_norm)
    grad_down[...] = (down[...] * factor).T
    grad_up[...] = (up[...] * factor).T


def clip(down, up, squares, clip_norm):
    rank = down.shape[0]
    shape = jax.ShapeDtypeStruct((LANES, rank), F32)
    return pl.pallas_call(
        functools.partial(clip_body, clip_norm=clip_norm),
        out_shape=(shape, shape),
        in_specs=vmem(3),
        out_specs=tuple(vmem(2)),
        name="clip",
    )(down, up, squares)


def tiles_of(order, fixed):
    names = [fixed]
    for mask in order:
        names = [n | b for n in names for b in (0, mask)]
    return names


def log2(n):
    assert n & (n - 1) == 0
    return n.bit_length() - 1


def local_blocks(hidden, score_direction, adapter_down, adapter_up, rewards, values, log_ratio, lengths):
    seq_count, shard_len, model_width = hidden.shape
    rank = adapter_down.shape[1]
    nb, ns = lax.axis_size("batch"), lax.axis_size("seq")
    count = nb * ns
    total_len = shard_len * ns
    shard = lax.axis_index("seq")
    hid, direction = hidden[0], score_direction[0]

    inner = jnp.arange(shard_len, dtype=jnp.int32)
    valid = (shard * shard_len + inner < lengths[0]).astype(F32)[None]
    live = rewards * valid
    first = jnp.sum(live * jnp.exp(-inner.astype(F32) / total_len)[None])
    group = jnp.full((8, LANES), first)
    carried = jnp.zeros((8, LANES), F32)
    for j in range(log2(ns)):
        side = 1 << j
        other = swap(group, side, count)
        upper = (shard & side) != 0
        steps = (side - 1 - (shard & (side - 1))).astype(F32)
        here = jnp.where(upper, 0.0, jnp.exp(-steps * shard_len / total_len))
        far = math.exp(-side * shard_len / total_len)
        carried = carried + here * other
        group = jnp.where(upper, other + far * group, group + far * other)

    down_t, up_t, within = project(hid, adapter_down, direction, adapter_up, live, total_len)
    returns, scaled_up, scaled_down = weigh(
        lengths, down_t, up_t, within, carried, values, log_ratio,
        shards=ns, total_len=total_len, seq_total=seq_count * nb,
    )

    ops = (hid, direction, scaled_up, scaled_down)
    seq_bits = [1 << j for j in range(log2(ns))]
    core, plane = seq_bits[0], seq_bits[1:]
    xs, ys = plane[: len(plane) // 2], plane[len(plane) // 2 :]
    zs = [ns << j for j in range(log2(nb))]
    cut = rank * 3 // 4
    colors = {
        "a": (xs + ys + zs, ((0, 0, cut),)),
        "b": (ys + xs + zs, ((1, 0, cut),)),
        "c": (zs + xs + ys, ((0, cut, rank - cut), (1, cut, rank - cut))),
    }
    sent, kept = {}, {}
    for name in colors:
        order, parts = colors[name]
        (theirs,) = blocks(ops, [(tiles_of(order[1:], order[0] | core), parts)], None, ns, "far_" + name)
        got = swap(theirs, core, count)
        (mine,) = blocks(ops, [(tiles_of(order[1:], order[0]), parts)], [got], ns, "near_" + name)
        sent[name] = swap(mine, order[0], count)
    theirs = blocks(ops, [(tiles_of(o[1:], core), p) for o, p in colors.values()], None, ns, "far_rest")
    got = [swap(t, core, count) for t in theirs]
    kept = dict(zip(colors, blocks(ops, [(tiles_of(o[1:], 0), p) for o, p in colors.values()], got, ns, "near_rest")))

    n_plane = len(plane)
    for i in range(1, len(plane) + len(zs)):
        if i < n_plane:
            for name in "ab":
                s, k = fold([(kept[name], sent[name])], f"fold_{name}{i}")
                kept[name], sent[name] = k, swap(s, colors[name][0][i], count)
        elif i == n_plane:
            s, k = fold([(kept[n], sent[n]) for n in "ab"], f"fold_ab{i}")
            kept["ab"], sent["ab"] = k, swap(s, colors["a"][0][i], count)
        else:
            s, k = fold([(kept["ab"], sent["ab"])], f"fold_ab{i}")
            kept["ab"], sent["ab"] = k, swap(s, colors["a"][0][i], count)
        s, k = fold([(kept["c"], sent["c"])], f"fold_c{i}")
        kept["c"], sent["c"] = k, swap(s, colors["c"][0][i], count)

    down, up, squares = total(kept["ab"], sent["ab"], kept["c"], sent["c"], cut, rank, count)
    squares = lax.all_to_all(squares, AXES, 0, 0, tiled=True)
    clip_norm = 0.5 * math.sqrt(2.0 * model_width * rank)
    grad_down, grad_up = clip(down, up, squares, clip_norm)
    return returns, grad_down, grad_up


def local_plain(hidden, score_direction, adapter_down, adapter_up, rewards, values, log_ratio, lengths):
    seq_count, shard_len, model_width = hidden.shape
    rank = adapter_down.shape[1]
    ns = lax.axis_size("seq")
    total_len = shard_len * ns
    seq_total = seq_count * lax.axis_size("batch")
    shard = lax.axis_index("seq")
    inner = jnp.arange(shard_len, dtype=jnp.int32)
    valid = ((shard * shard_len + inner)[None, :] < lengths[:, None]).astype(F32)
    scale = 1.0 / math.sqrt(rank)
    down = jnp.einsum("ogz,zw->ogw", hidden, adapter_down, preferred_element_type=F32)
    up = jnp.einsum("ogz,zw->ogw", score_direction, adapter_up, preferred_element_type=F32)
    importance = jnp.exp(log_ratio + scale * jnp.sum(down * up, axis=-1))
    live = rewards * valid
    offsets = (inner[None, :] - inner[:, None]).astype(F32)
    discount = jnp.where(offsets >= 0, jnp.exp(-offsets / total_len), jnp.zeros_like(offsets))
    within = jnp.einsum("sk,tk->st", live, discount, precision=lax.Precision.HIGHEST)
    firsts = lax.all_gather(within[:, :1], "seq", axis=1, tiled=True)
    index = jnp.arange(ns, dtype=jnp.int32)
    steps = (index - shard - 1).astype(F32)
    here = jnp.where(index > shard, jnp.exp(-steps * shard_len / total_len), jnp.zeros_like(steps))
    carried = jnp.sum(firsts * here[None, :], axis=1)
    tail = jnp.exp(-(shard_len - inner).astype(F32) / total_len)
    returns = within + tail[None, :] * carried[:, None]
    gain = weight_gain * math.sqrt(total_len * rank / seq_total) / lengths.astype(F32)
    weight = valid * jnp.minimum(importance, ratio_cap) * (returns - values) * gain[:, None]
    scaled_up = (-scale * weight[:, :, None] * up).astype(jnp.bfloat16)
    scaled_down = (-scale * weight[:, :, None] * down).astype(jnp.bfloat16)
    terms = jnp.concatenate(
        [
            jnp.einsum("oxe,oxq->eq", hidden, scaled_up, preferred_element_type=F32),
            jnp.einsum("oxe,oxq->eq", score_direction, scaled_down, preferred_element_type=F32),
        ],
        axis=1,
    )
    own = lax.psum_scatter(terms, AXES, scatter_dimension=0, tiled=True)
    norm = jnp.sqrt(lax.psum(jnp.sum(own * own), AXES))
    clip_norm = 0.5 * math.sqrt(2.0 * model_width * rank)
    factor = clip_norm / jnp.maximum(norm, clip_norm)
    return returns, own[:, :rank] * factor, own[:, rank:] * factor


def solution(mesh):
    placed = (
        P("batch", "seq", None),
        P("batch", "seq", None),
        P(),
        P(),
        P("batch", "seq"),
        P("batch", "seq"),
        P("batch", "seq"),
        P("batch"),
    )
    nb, ns = mesh.shape["batch"], mesh.shape["seq"]

    def step(hidden, *rest):
        powers = nb & (nb - 1) == 0 and ns & (ns - 1) == 0 and nb >= 2 and ns >= 8
        blocked = powers and hidden.shape[0] == nb and hidden.shape[2] == nb * ns * LANES
        return jax.shard_map(
            local_blocks if blocked else local_plain,
            mesh=mesh,
            in_specs=placed,
            out_specs=(P("batch", "seq"), P(AXES, None), P(AXES, None)),
            check_vma=False,
        )(hidden, *rest)

    return step
```

```python
import functools
import math

import jax
import jax.numpy as jnp
from jax import lax
from jax.experimental import pallas as pl
from jax.experimental.pallas import tpu as pltpu
from jax.sharding import PartitionSpec as P


ratio_cap = 2.0
weight_gain = 0.08
AXES = ("batch", "seq")
LANES = 128
KERNEL_VMEM = 8 * 1024 * 1024
F32 = jnp.float32

PARTS = (("xzy", 12), ("yxz", 12), ("zyx", 12), ("yxz", 15), ("xyz", 13))
TURNS = (0, 2, 1, 4, 0, 3, 1, 4, 2, 0, 3, 4, 1, 3, 2)

SMEM = pl.BlockSpec(memory_space=pltpu.SMEM)
VMEM = pl.BlockSpec(memory_space=pltpu.VMEM)
HBM = pl.BlockSpec(memory_space=pltpu.HBM)


def swap(x, mask, count):
    return lax.ppermute(x, AXES, [(i, i ^ mask) for i in range(count)])


class Line:
    def __init__(self):
        self.token = None

    def call(self, body, outs, ins, scalars=(), from_hbm=(), scratch=(), in_vmem=True):
        first = self.token is None
        n_in = len(scalars) + len(from_hbm) + len(ins)

        def run(*refs):
            given, refs = refs[:n_in], refs[n_in:]
            if not first:
                refs = refs[1:]
            made, token, rest = refs[: len(outs)], refs[len(outs)], refs[len(outs) + 1 :]
            body(*given, *made, *rest)
            token[...] = jnp.zeros_like(token)

        kind = pltpu.VMEM if in_vmem else jax.ShapeDtypeStruct
        tokens = [] if first else [self.token]
        kernel = pl.pallas_call(
            run,
            out_shape=(*[kind(*o) for o in outs], pltpu.VMEM((8, LANES), F32)),
            in_specs=[SMEM] * len(scalars) + [HBM] * len(from_hbm) + [VMEM] * (len(ins) + len(tokens)),
            out_specs=(VMEM,) * (len(outs) + 1),
            scratch_shapes=list(scratch),
            compiler_params=pltpu.CompilerParams(vmem_limit_bytes=KERNEL_VMEM),
        )
        from_hbm = [pltpu.with_memory_space_constraint(x, pltpu.HBM) for x in from_hbm]
        ins = [pltpu.with_memory_space_constraint(x, pltpu.VMEM) for x in [*ins, *tokens]]
        *got, self.token = kernel(*scalars, *from_hbm, *ins)
        return got


def row_of(tokens):
    return lax.broadcasted_iota(jnp.int32, (1, tokens), 1)


def first_body(length, rewards, live, group, *, total_len):
    tokens = rewards.shape[1]
    at = row_of(tokens)
    valid = jnp.where(at + lax.axis_index("seq") * tokens < length[0], 1.0, 0.0)
    row = rewards[...] * valid * jnp.exp(-at.astype(F32) / total_len)
    live[...] = row
    group[...] = jnp.broadcast_to(jnp.sum(row, axis=1, keepdims=True), group.shape)


def carry(group, other, carried, side, tokens, total_len):
    shard = lax.axis_index("seq")
    upper = jnp.full(group.shape, shard & side, jnp.int32) != 0
    steps = jnp.full(group.shape, side - 1 - (shard & (side - 1)), jnp.int32).astype(F32)
    here = jnp.where(upper, 0.0, jnp.exp(-steps * (tokens / total_len)))
    far = math.exp(-side * tokens / total_len)
    return jnp.where(upper, other + far * group, group + far * other), carried + here * other


def carry_body(group, other, carried, new_group, new_carried, **sizes):
    new_group[...], new_carried[...] = carry(group[...], other[...], carried[...], **sizes)


def project_body(src_hbm, mat_hbm, src, out_t, mat, acc, src_sems, mat_sems, *, steps):
    width = src.shape[1]
    step = width // steps
    copies = []
    for i in range(steps):
        cut = pl.ds(i * step, step)
        copies.append(pltpu.make_async_copy(src_hbm.at[:, cut], src.at[:, cut], src_sems.at[i]))
        copies.append(pltpu.make_async_copy(mat_hbm.at[cut, :], mat.at[cut, :], mat_sems.at[i]))
    for c in copies:
        c.start()
    for i in range(steps):
        copies[2 * i].wait()
        copies[2 * i + 1].wait()
        cut = slice(i * step, (i + 1) * step)
        part = jnp.dot(src[:, cut], mat[cut, :], preferred_element_type=F32)
        if i:
            part = part + acc[...]
        if i < steps - 1:
            acc[...] = part
        else:
            out_t[...] = part.T


def within_of(row, total_len):
    tokens = row.shape[1]
    first = row.astype(jnp.bfloat16)
    rest = row - first.astype(F32)
    second = rest.astype(jnp.bfloat16)
    third = (rest - second.astype(F32)).astype(jnp.bfloat16)
    rows = jnp.concatenate([first, second, third], axis=0)
    k_of = lax.broadcasted_iota(jnp.int32, (tokens, tokens), 0)
    t_of = lax.broadcasted_iota(jnp.int32, (tokens, tokens), 1)
    sums = jnp.dot(rows, (k_of >= t_of).astype(jnp.bfloat16), preferred_element_type=F32)
    return jnp.sum(sums, axis=0, keepdims=True) * jnp.exp(row_of(tokens).astype(F32) / total_len)


def within_body(row, within, *, total_len):
    within[...] = within_of(row[...], total_len)


def weigh_body(
    length, down_t, up_t, within, group, other, carried, values, log_ratio,
    returns, scaled_up, scaled_down, *, side, total_len, seq_total,
):
    rank, tokens = down_t.shape
    at = row_of(tokens)
    _, incoming = carry(group[...], other[...], carried[...], side, tokens, total_len)
    tail = jnp.exp((at - tokens).astype(F32) / total_len)
    back = within[...] + tail * incoming[0:1, 0:1]
    returns[...] = back
    adapter_scale = 1.0 / math.sqrt(rank)
    delta = adapter_scale * jnp.sum(down_t[...] * up_t[...], axis=0, keepdims=True)
    importance = jnp.exp(log_ratio[...] + delta)
    count = length[0]
    lens = jnp.full((1, tokens), count, jnp.int32).astype(F32)
    gain = weight_gain * math.sqrt(total_len * rank / seq_total) / lens
    valid = jnp.where(at + lax.axis_index("seq") * tokens < count, 1.0, 0.0)
    weight = -adapter_scale * (valid * jnp.minimum(importance, ratio_cap) * (back - values[...]) * gain)
    scaled_up[...] = (weight * up_t[...]).astype(jnp.bfloat16)
    scaled_down[...] = (weight * down_t[...]).astype(jnp.bfloat16)


def blocks_body(*refs, jobs, seq_size, n_out, adds):
    hid, direction, scaled_up, scaled_down = refs[:4]
    received = refs[4 : 4 + n_out] if adds else ()
    outs = refs[4 + n_out :] if adds else refs[4:]
    me = lax.axis_index("batch") * seq_size + lax.axis_index("seq")
    for out_at, tiles, row_at, rows, side, from_row in jobs:
        src, weight = ((hid, scaled_up), (direction, scaled_down))[side]
        out = outs[out_at]
        for i in range(0, len(tiles), 2):
            pair = tiles[i : i + 2]
            cols = [src[:, pl.ds(pl.multiple_of((t ^ me) * LANES, LANES), LANES)] for t in pair]
            block = jnp.concatenate(cols, axis=1) if len(cols) > 1 else cols[0]
            grad = jnp.dot(weight[from_row : from_row + rows, :], block, preferred_element_type=F32)
            for j in range(len(pair)):
                part = grad[:, j * LANES : (j + 1) * LANES]
                if adds:
                    part = part + received[out_at][i + j, row_at : row_at + rows, :]
                out[i + j, row_at : row_at + rows, :] = part


def blocks(line, ops, wanted, received, seq_size):
    jobs, shapes = [], []
    for out_at, (tiles, pieces) in enumerate(wanted):
        at = 0
        for side, from_row, rows in pieces:
            jobs.append((out_at, tuple(tiles), at, rows, side, from_row))
            at += rows
        shapes.append(((len(tiles), at, LANES), F32))
    extra = tuple(received) if received is not None else ()
    body = functools.partial(
        blocks_body, jobs=tuple(jobs), seq_size=seq_size, n_out=len(wanted), adds=received is not None
    )
    return line.call(body, shapes, (*ops, *extra))


def fold_body(keep, got, send, left):
    half = send.shape[0]
    send[...] = keep[half:] + got[half:]
    left[...] = keep[:half] + got[:half]


def total_body(*refs, n, rank):
    keeps, gots, (down, up, squares) = refs[:n], refs[n : 2 * n], refs[2 * n :]
    at, row = 0, 0.0
    for keep, got in zip(keeps, gots):
        part = keep[0] + got[0]
        row = row + jnp.sum(part * part, axis=0, keepdims=True)
        rows = part.shape[0]
        split = min(max(rank - at, 0), rows)
        if split:
            down[at : at + split, :] = part[:split]
        if split < rows:
            up[at + split - rank : at + rows - rank, :] = part[split:]
        at += rows
    squares[...] = jnp.broadcast_to(row[None], squares.shape)


def clip_body(down, up, squares, grad_down, grad_up, *, clip_norm):
    norm = jnp.sqrt(jnp.sum(jnp.sum(squares[...], axis=0), axis=1, keepdims=True))
    factor = clip_norm / jnp.maximum(norm, clip_norm)
    grad_down[...] = (down[...] * factor).T
    grad_up[...] = (up[...] * factor).T


def tiles_of(order, fixed):
    names = [fixed]
    for mask in order:
        names = [n | b for n in names for b in (0, mask)]
    return names


def log2(n):
    return n.bit_length() - 1


def turns_of(halvings):
    n = len(PARTS)
    return TURNS if len(TURNS) == n * (halvings - 1) else [i for _ in range(halvings - 1) for i in range(n)]


def local_blocks(hidden, score_direction, adapter_down, adapter_up, rewards, values, log_ratio, lengths):
    return in_blocks(hidden, score_direction, adapter_down, adapter_up, rewards, values, log_ratio, lengths)


def in_blocks(hidden, score_direction, adapter_down, adapter_up, rewards, values, log_ratio, lengths):
    _, tokens, width = hidden.shape
    rank = adapter_down.shape[1]
    nb, ns = lax.axis_size("batch"), lax.axis_size("seq")
    count = nb * ns
    total_len = tokens * ns
    hid_hbm, direction_hbm = hidden[0], score_direction[0]
    line = Line()

    bits = [1 << j for j in range(log2(ns))]
    tile = ((8, LANES), F32)
    live, group = line.call(
        functools.partial(first_body, total_len=total_len), [((1, tokens), F32), tile], (rewards,), (lengths,)
    )
    carried = jnp.zeros(*tile)
    steps = 8
    under = [(hid_hbm, adapter_down), (direction_hbm, adapter_up)]
    made = []
    for j, side in enumerate(bits):
        other = swap(group, side, count)
        if j == 0:
            (within,) = line.call(functools.partial(within_body, total_len=total_len), [((1, tokens), F32)], (live,))
        if j >= len(bits) - len(under):
            src, mat = under[len(made)]
            made.append(
                line.call(
                    functools.partial(project_body, steps=steps),
                    [((tokens, width), src.dtype), ((rank, tokens), F32)],
                    (),
                    from_hbm=(src, mat),
                    scratch=[
                        pltpu.VMEM((width, rank), mat.dtype),
                        pltpu.VMEM((tokens, rank), F32),
                        pltpu.SemaphoreType.DMA((steps,)),
                        pltpu.SemaphoreType.DMA((steps,)),
                    ],
                )
            )
        if j < len(bits) - 1:
            group, carried = line.call(
                functools.partial(carry_body, side=side, tokens=tokens, total_len=total_len),
                [tile, tile], (group, other, carried),
            )
    (hid, down_t), (direction, up_t) = made
    returns, scaled_up, scaled_down = line.call(
        functools.partial(weigh_body, side=bits[-1], total_len=total_len, seq_total=nb),
        [((1, tokens), F32), ((rank, tokens), jnp.bfloat16), ((rank, tokens), jnp.bfloat16)],
        (down_t, up_t, within, group, other, carried, values, log_ratio), (lengths,),
    )

    ops = (hid, direction, scaled_up, scaled_down)
    core, plane = bits[0], bits[1:]
    masks = {"x": plane[: len(plane) // 2], "y": plane[len(plane) // 2 :], "z": [ns << j for j in range(log2(nb))]}
    orders, pieces, at = [], [], 0
    for axes, share in PARTS:
        orders.append([m for axis in axes for m in masks[axis]])
        end = at + 2 * rank * share // 64
        pieces.append([
            (side, max(at - side * rank, 0), min(end, rank * (side + 1)) - max(at, rank * side))
            for side in (0, 1)
            if min(end, rank * (side + 1)) > max(at, rank * side)
        ])
        at = end
    n = len(PARTS)
    sends = [(tiles_of(orders[i][1:], orders[i][0]), pieces[i]) for i in range(n)]
    stays = [(tiles_of(orders[i][1:], 0), pieces[i]) for i in range(n)]
    far = lambda w: ([t | core for t in w[0]], w[1])
    got, sent, theirs = [None] * n, [None] * n, [None] * n
    for i in range(n + 1):
        if i < n:
            (theirs[i],) = blocks(line, ops, [far(sends[i])], None, ns)
            got[i] = swap(theirs[i], core, count)
        if i:
            (mine,) = blocks(line, ops, [sends[i - 1]], [got[i - 1]], ns)
            sent[i - 1] = swap(mine, orders[i - 1][0], count)
    got = [swap(t, core, count) for t in blocks(line, ops, [far(w) for w in stays], None, ns)]
    kept = blocks(line, ops, stays, got, ns)

    taken = [1] * n
    for i in turns_of(len(orders[0])):
        blocks_now, rows, _ = kept[i].shape
        send, kept[i] = line.call(fold_body, [((blocks_now // 2, rows, LANES), F32)] * 2, (kept[i], sent[i]))
        sent[i] = swap(send, orders[i][taken[i]], count)
        taken[i] += 1

    down, up, squares = line.call(
        functools.partial(total_body, n=n, rank=rank),
        [((rank, LANES), F32), ((rank, LANES), F32), ((count, 1, LANES), F32)], (*kept, *sent),
    )
    squares = lax.all_to_all(squares, AXES, 0, 0, tiled=True)
    clip_norm = 0.5 * math.sqrt(2.0 * width * rank)
    grad_down, grad_up = line.call(
        functools.partial(clip_body, clip_norm=clip_norm), [((LANES, rank), F32)] * 2, (down, up, squares), in_vmem=False
    )
    return returns, grad_down, grad_up


def local_plain(hidden, score_direction, adapter_down, adapter_up, rewards, values, log_ratio, lengths):
    seq_count, shard_len, model_width = hidden.shape
    rank = adapter_down.shape[1]
    ns = lax.axis_size("seq")
    total_len = shard_len * ns
    seq_total = seq_count * lax.axis_size("batch")
    shard = lax.axis_index("seq")
    inner = jnp.arange(shard_len, dtype=jnp.int32)
    valid = ((shard * shard_len + inner)[None, :] < lengths[:, None]).astype(F32)
    scale = 1.0 / math.sqrt(rank)
    down = jnp.einsum("ogz,zw->ogw", hidden, adapter_down, preferred_element_type=F32)
    up = jnp.einsum("ogz,zw->ogw", score_direction, adapter_up, preferred_element_type=F32)
    importance = jnp.exp(log_ratio + scale * jnp.sum(down * up, axis=-1))
    live = rewards * valid
    offsets = (inner[None, :] - inner[:, None]).astype(F32)
    discount = jnp.where(offsets >= 0, jnp.exp(-offsets / total_len), jnp.zeros_like(offsets))
    within = jnp.einsum("sk,tk->st", live, discount, precision=lax.Precision.HIGHEST)
    firsts = lax.all_gather(within[:, :1], "seq", axis=1, tiled=True)
    index = jnp.arange(ns, dtype=jnp.int32)
    steps = (index - shard - 1).astype(F32)
    here = jnp.where(index > shard, jnp.exp(-steps * shard_len / total_len), jnp.zeros_like(steps))
    carried = jnp.sum(firsts * here[None, :], axis=1)
    tail = jnp.exp(-(shard_len - inner).astype(F32) / total_len)
    returns = within + tail[None, :] * carried[:, None]
    gain = weight_gain * math.sqrt(total_len * rank / seq_total) / lengths.astype(F32)
    weight = valid * jnp.minimum(importance, ratio_cap) * (returns - values) * gain[:, None]
    scaled_up = (-scale * weight[:, :, None] * up).astype(jnp.bfloat16)
    scaled_down = (-scale * weight[:, :, None] * down).astype(jnp.bfloat16)
    terms = jnp.concatenate(
        [
            jnp.einsum("oxe,oxq->eq", hidden, scaled_up, preferred_element_type=F32),
            jnp.einsum("oxe,oxq->eq", score_direction, scaled_down, preferred_element_type=F32),
        ],
        axis=1,
    )
    own = lax.psum_scatter(terms, AXES, scatter_dimension=0, tiled=True)
    norm = jnp.sqrt(lax.psum(jnp.sum(own * own), AXES))
    clip_norm = 0.5 * math.sqrt(2.0 * model_width * rank)
    factor = clip_norm / jnp.maximum(norm, clip_norm)
    return returns, own[:, :rank] * factor, own[:, rank:] * factor


def solution(mesh):
    placed = (
        P("batch", "seq", None),
        P("batch", "seq", None),
        P(),
        P(),
        P("batch", "seq"),
        P("batch", "seq"),
        P("batch", "seq"),
        P("batch"),
    )
    nb, ns = mesh.shape["batch"], mesh.shape["seq"]

    def step(hidden, *rest):
        powers = nb & (nb - 1) == 0 and ns & (ns - 1) == 0 and nb >= 2 and ns >= 8
        blocked = powers and hidden.shape[0] == nb and hidden.shape[2] == nb * ns * LANES
        return jax.shard_map(
            local_blocks if blocked else local_plain,
            mesh=mesh,
            in_specs=placed,
            out_specs=(P("batch", "seq"), P(AXES, None), P(AXES, None)),
            check_vma=False,
        )(hidden, *rest)

    return step
```

```python
import functools
import math

import jax
import jax.numpy as jnp
from jax import lax
from jax.experimental import pallas as pl
from jax.experimental.pallas import tpu as pltpu
from jax.sharding import PartitionSpec as P


ratio_cap = 2.0
weight_gain = 0.08
AXES = ("batch", "seq")
LANES = 128
KERNEL_VMEM = 8 * 1024 * 1024
F32 = jnp.float32

PARTS = (("zxyw", 19), ("yxzw", 17), ("xyzw", 16), ("wyzx", 12))
TURNS = (1, 2, 0, 2, 3, 1, 2, 0, 3, 1, 0, 3)

SMEM = pl.BlockSpec(memory_space=pltpu.SMEM)
VMEM = pl.BlockSpec(memory_space=pltpu.VMEM)
HBM = pl.BlockSpec(memory_space=pltpu.HBM)


def swap(x, mask, count):
    return lax.ppermute(x, AXES, [(i, i ^ mask) for i in range(count)])


class Line:
    def __init__(self):
        self.token = None
        self.placed = {}

    def place(self, x):
        x = pltpu.with_memory_space_constraint(x, pltpu.VMEM)
        self.placed[id(x)] = x
        return x

    def call(self, body, outs, ins, scalars=(), from_hbm=(), scratch=(), in_vmem=True, flops=0):
        first = self.token is None
        n_in = len(scalars) + len(from_hbm) + len(ins)

        def run(*refs):
            given, refs = refs[:n_in], refs[n_in:]
            if not first:
                refs = refs[1:]
            made, token, rest = refs[: len(outs)], refs[len(outs)], refs[len(outs) + 1 :]
            body(*given, *made, *rest)
            token[...] = jnp.zeros_like(token)

        kind = pltpu.VMEM if in_vmem else jax.ShapeDtypeStruct
        tokens = [] if first else [self.token]
        kernel = pl.pallas_call(
            run,
            out_shape=(*[kind(*o) for o in outs], pltpu.VMEM((8, LANES), F32)),
            in_specs=[SMEM] * len(scalars) + [HBM] * len(from_hbm) + [VMEM] * (len(ins) + len(tokens)),
            out_specs=(VMEM,) * (len(outs) + 1),
            scratch_shapes=list(scratch),
            compiler_params=pltpu.CompilerParams(vmem_limit_bytes=KERNEL_VMEM),
            cost_estimate=pl.CostEstimate(flops=flops, bytes_accessed=0, transcendentals=0) if flops else None,
        )
        from_hbm = [pltpu.with_memory_space_constraint(x, pltpu.HBM) for x in from_hbm]
        ins = [x if id(x) in self.placed else pltpu.with_memory_space_constraint(x, pltpu.VMEM) for x in [*ins, *tokens]]
        *got, self.token = kernel(*scalars, *from_hbm, *ins)
        return got


def row_of(tokens):
    return lax.broadcasted_iota(jnp.int32, (1, tokens), 1)


def first_body(length, rewards, live, group, *, total_len):
    tokens = rewards.shape[1]
    at = row_of(tokens)
    valid = jnp.where(at + lax.axis_index("seq") * tokens < length[0], 1.0, 0.0)
    row = rewards[...] * valid * jnp.exp(-at.astype(F32) / total_len)
    live[...] = row
    group[...] = jnp.broadcast_to(jnp.sum(row, axis=1, keepdims=True), group.shape)


def carry(group, other, carried, side, tokens, total_len):
    shard = lax.axis_index("seq")
    upper = jnp.full(group.shape, shard & side, jnp.int32) != 0
    steps = jnp.full(group.shape, side - 1 - (shard & (side - 1)), jnp.int32).astype(F32)
    here = jnp.where(upper, 0.0, jnp.exp(-steps * (tokens / total_len)))
    far = math.exp(-side * tokens / total_len)
    return jnp.where(upper, other + far * group, group + far * other), carried + here * other


def carry_body(group, other, carried, new_group, new_carried, **sizes):
    new_group[...], new_carried[...] = carry(group[...], other[...], carried[...], **sizes)


def project_body(src, mat, out_t, acc, *, steps):
    step = src.shape[1] // steps
    for i in range(steps):
        cut = slice(i * step, (i + 1) * step)
        part = jnp.dot(src[:, cut], mat[cut, :], preferred_element_type=F32)
        if i:
            part = part + acc[...]
        if i < steps - 1:
            acc[...] = part
        else:
            out_t[...] = part.T


def within_of(row, total_len):
    tokens = row.shape[1]
    first = row.astype(jnp.bfloat16)
    rest = row - first.astype(F32)
    second = rest.astype(jnp.bfloat16)
    third = (rest - second.astype(F32)).astype(jnp.bfloat16)
    rows = jnp.concatenate([first, second, third], axis=0)
    k_of = lax.broadcasted_iota(jnp.int32, (tokens, tokens), 0)
    t_of = lax.broadcasted_iota(jnp.int32, (tokens, tokens), 1)
    sums = jnp.dot(rows, (k_of >= t_of).astype(jnp.bfloat16), preferred_element_type=F32)
    return jnp.sum(sums, axis=0, keepdims=True) * jnp.exp(row_of(tokens).astype(F32) / total_len)


def within_body(row, within, *, total_len):
    within[...] = within_of(row[...], total_len)


def weigh_body(
    length, down_t, up_t, within, group, other, carried, values, log_ratio,
    returns, scaled_up, scaled_down, *, side, total_len, seq_total,
):
    rank, tokens = down_t.shape
    at = row_of(tokens)
    _, incoming = carry(group[...], other[...], carried[...], side, tokens, total_len)
    tail = jnp.exp((at - tokens).astype(F32) / total_len)
    back = within[...] + tail * incoming[0:1, 0:1]
    returns[...] = back
    adapter_scale = 1.0 / math.sqrt(rank)
    delta = adapter_scale * jnp.sum(down_t[...] * up_t[...], axis=0, keepdims=True)
    importance = jnp.exp(log_ratio[...] + delta)
    count = length[0]
    lens = jnp.full((1, tokens), count, jnp.int32).astype(F32)
    gain = weight_gain * math.sqrt(total_len * rank / seq_total) / lens
    valid = jnp.where(at + lax.axis_index("seq") * tokens < count, 1.0, 0.0)
    weight = -adapter_scale * (valid * jnp.minimum(importance, ratio_cap) * (back - values[...]) * gain)
    scaled_up[...] = (weight * up_t[...]).astype(jnp.bfloat16)
    scaled_down[...] = (weight * down_t[...]).astype(jnp.bfloat16)


def blocks_body(*refs, jobs, seq_size):
    hid, direction, scaled_up, scaled_down, *outs = refs
    me = lax.axis_index("batch") * seq_size + lax.axis_index("seq")
    for out_at, tiles, row_at, rows, side, from_row in jobs:
        src, weight = ((hid, scaled_up), (direction, scaled_down))[side]
        out = outs[out_at]
        for i in range(0, len(tiles), 2):
            pair = tiles[i : i + 2]
            cols = [src[:, pl.ds(pl.multiple_of((t ^ me) * LANES, LANES), LANES)] for t in pair]
            block = jnp.concatenate(cols, axis=1) if len(cols) > 1 else cols[0]
            grad = jnp.dot(weight[from_row : from_row + rows, :], block, preferred_element_type=F32)
            for j in range(len(pair)):
                out[i + j, row_at : row_at + rows, :] = grad[:, j * LANES : (j + 1) * LANES]


def blocks(line, ops, wanted, seq_size):
    jobs, shapes = [], []
    for out_at, (tiles, pieces) in enumerate(wanted):
        at = 0
        for side, from_row, rows in pieces:
            jobs.append((out_at, tuple(tiles), at, rows, side, from_row))
            at += rows
        shapes.append(((len(tiles), at, LANES), F32))
    return line.call(functools.partial(blocks_body, jobs=tuple(jobs), seq_size=seq_size), shapes, ops)


def add_body(a, b, out):
    out[...] = a[...] + b[...]


def fold_body(*refs):
    *terms, send, left = refs
    half = send.shape[0]
    send[...] = functools.reduce(jnp.add, [t[half:] for t in terms])
    left[...] = functools.reduce(jnp.add, [t[:half] for t in terms])


def total_body(*refs, n, rank):
    keeps, gots, (down, up, squares) = refs[:n], refs[n : 2 * n], refs[2 * n :]
    at, row = 0, 0.0
    for keep, got in zip(keeps, gots):
        part = keep[0] + got[0]
        row = row + jnp.sum(part * part, axis=0, keepdims=True)
        rows = part.shape[0]
        split = min(max(rank - at, 0), rows)
        if split:
            down[at : at + split, :] = part[:split]
        if split < rows:
            up[at + split - rank : at + rows - rank, :] = part[split:]
        at += rows
    squares[...] = jnp.broadcast_to(row[None], squares.shape)


def clip_body(down, up, squares, grad_down, grad_up, *, clip_norm):
    norm = jnp.sqrt(jnp.sum(jnp.sum(squares[...], axis=0), axis=1, keepdims=True))
    factor = clip_norm / jnp.maximum(norm, clip_norm)
    grad_down[...] = (down[...] * factor).T
    grad_up[...] = (up[...] * factor).T


def tiles_of(order, fixed):
    names = [fixed]
    for mask in order:
        names = [n | b for n in names for b in (0, mask)]
    return names


def log2(n):
    return n.bit_length() - 1


def script(halvings):
    n = len(PARTS)
    first = list(range(n))
    steps = [("blocks", 0, 0)]
    for i in first:
        steps += [("blocks", i + 1, 0), ("add", i, 0)]
    steps += [("far_rest", 0, 0), ("near_rest", 0, 0)]
    turns = TURNS if len(TURNS) == n * (halvings - 1) else first * (halvings - 1)
    taken = [1] * n
    for i in turns:
        steps.append(("fold", i, taken[i]))
        taken[i] += 1
    return steps


def local_blocks(hidden, score_direction, adapter_down, adapter_up, rewards, values, log_ratio, lengths):
    return in_blocks(hidden, score_direction, adapter_down, adapter_up, rewards, values, log_ratio, lengths)


def in_blocks(hidden, score_direction, adapter_down, adapter_up, rewards, values, log_ratio, lengths):
    _, tokens, width = hidden.shape
    rank = adapter_down.shape[1]
    nb, ns = lax.axis_size("batch"), lax.axis_size("seq")
    count = nb * ns
    total_len = tokens * ns
    hid_hbm, direction_hbm = hidden[0], score_direction[0]
    line = Line()

    bits = [1 << j for j in range(log2(ns))]
    tile = ((8, LANES), F32)
    FL = 40_000_000_000
    live, group = line.call(
        functools.partial(first_body, total_len=total_len), [((1, tokens), F32), tile], (rewards,), (lengths,)
    )
    carried = jnp.zeros(*tile)
    hid, direction = line.place(hid_hbm), line.place(direction_hbm)
    under = [(hid, adapter_down), (direction, adapter_up)]
    made = []
    for j, side in enumerate(bits):
        other = swap(group, side, count)
        if j == 0:
            (within,) = line.call(functools.partial(within_body, total_len=total_len), [((1, tokens), F32)], (live,), flops=FL)
        if j >= len(bits) - len(under):
            (proj,) = line.call(
                functools.partial(project_body, steps=2),
                [((rank, tokens), F32)],
                under[len(made)],
                scratch=[pltpu.VMEM((tokens, rank), F32)],
            )
            made.append(proj)
        if j < len(bits) - 1:
            group, carried = line.call(
                functools.partial(carry_body, side=side, tokens=tokens, total_len=total_len),
                [tile, tile], (group, other, carried),
            )
    down_t, up_t = made
    returns, scaled_up, scaled_down = line.call(
        functools.partial(weigh_body, side=bits[-1], total_len=total_len, seq_total=nb),
        [((1, tokens), F32), ((rank, tokens), jnp.bfloat16), ((rank, tokens), jnp.bfloat16)],
        (down_t, up_t, within, group, other, carried, values, log_ratio), (lengths,),
    )

    ops = (hid, direction, scaled_up, scaled_down)
    core, plane = bits[0], bits[1:]
    zs = [ns << j for j in range(log2(nb))]
    masks = {"x": plane[: len(plane) // 2], "y": plane[len(plane) // 2 :], "z": zs[:-1], "w": zs[-1:]}
    orders, pieces, at = [], [], 0
    for axes, share in PARTS:
        orders.append([m for axis in axes for m in masks[axis]])
        end = at + 2 * rank * share // 64
        pieces.append([
            (side, max(at - side * rank, 0), min(end, rank * (side + 1)) - max(at, rank * side))
            for side in (0, 1)
            if min(end, rank * (side + 1)) > max(at, rank * side)
        ])
        at = end
    n = len(PARTS)
    sends = [(tiles_of(orders[i][1:], orders[i][0]), pieces[i]) for i in range(n)]
    stays = [(tiles_of(orders[i][1:], 0), pieces[i]) for i in range(n)]
    far = lambda w: ([t | core for t in w[0]], w[1])
    got, near, sent, kept = [None] * n, [None] * n, [None] * n, [None] * n
    for name, i, k in script(len(orders[0])):
        if name == "blocks":
            want = ([sends[i - 1]] if i else []) + ([far(sends[i])] if i < n else [])
            made = list(blocks(line, ops, want, ns))
            if i:
                near[i - 1] = made.pop(0)
            if i < n:
                got[i] = swap(made[0], core, count)
        elif name == "far_rest":
            rest = [swap(t, core, count) for t in blocks(line, ops, [far(w) for w in stays], ns)]
        elif name == "near_rest":
            kept = [(a, b) for a, b in zip(blocks(line, ops, stays, ns), rest)]
        else:
            if name == "add":
                (send,) = line.call(add_body, [(near[i].shape, F32)], (near[i], got[i]))
            else:
                terms = (*kept[i], sent[i])
                blocks_now, rows, _ = terms[0].shape
                send, left = line.call(fold_body, [((blocks_now // 2, rows, LANES), F32)] * 2, terms)
                kept[i] = (left,)
            sent[i] = swap(send, orders[i][k], count)

    down, up, squares = line.call(
        functools.partial(total_body, n=n, rank=rank),
        [((rank, LANES), F32), ((rank, LANES), F32), ((count, 1, LANES), F32)], (*[k[0] for k in kept], *sent),
    )
    squares = lax.all_to_all(squares, AXES, 0, 0, tiled=True)
    clip_norm = 0.5 * math.sqrt(2.0 * width * rank)
    grad_down, grad_up = line.call(
        functools.partial(clip_body, clip_norm=clip_norm), [((LANES, rank), F32)] * 2, (down, up, squares), in_vmem=False
    )
    return returns, grad_down, grad_up


def local_plain(hidden, score_direction, adapter_down, adapter_up, rewards, values, log_ratio, lengths):
    seq_count, shard_len, model_width = hidden.shape
    rank = adapter_down.shape[1]
    ns = lax.axis_size("seq")
    total_len = shard_len * ns
    seq_total = seq_count * lax.axis_size("batch")
    shard = lax.axis_index("seq")
    inner = jnp.arange(shard_len, dtype=jnp.int32)
    valid = ((shard * shard_len + inner)[None, :] < lengths[:, None]).astype(F32)
    scale = 1.0 / math.sqrt(rank)
    down = jnp.einsum("ogz,zw->ogw", hidden, adapter_down, preferred_element_type=F32)
    up = jnp.einsum("ogz,zw->ogw", score_direction, adapter_up, preferred_element_type=F32)
    importance = jnp.exp(log_ratio + scale * jnp.sum(down * up, axis=-1))
    live = rewards * valid
    offsets = (inner[None, :] - inner[:, None]).astype(F32)
    discount = jnp.where(offsets >= 0, jnp.exp(-offsets / total_len), jnp.zeros_like(offsets))
    within = jnp.einsum("sk,tk->st", live, discount, precision=lax.Precision.HIGHEST)
    firsts = lax.all_gather(within[:, :1], "seq", axis=1, tiled=True)
    index = jnp.arange(ns, dtype=jnp.int32)
    steps = (index - shard - 1).astype(F32)
    here = jnp.where(index > shard, jnp.exp(-steps * shard_len / total_len), jnp.zeros_like(steps))
    carried = jnp.sum(firsts * here[None, :], axis=1)
    tail = jnp.exp(-(shard_len - inner).astype(F32) / total_len)
    returns = within + tail[None, :] * carried[:, None]
    gain = weight_gain * math.sqrt(total_len * rank / seq_total) / lengths.astype(F32)
    weight = valid * jnp.minimum(importance, ratio_cap) * (returns - values) * gain[:, None]
    scaled_up = (-scale * weight[:, :, None] * up).astype(jnp.bfloat16)
    scaled_down = (-scale * weight[:, :, None] * down).astype(jnp.bfloat16)
    terms = jnp.concatenate(
        [
            jnp.einsum("oxe,oxq->eq", hidden, scaled_up, preferred_element_type=F32),
            jnp.einsum("oxe,oxq->eq", score_direction, scaled_down, preferred_element_type=F32),
        ],
        axis=1,
    )
    own = lax.psum_scatter(terms, AXES, scatter_dimension=0, tiled=True)
    norm = jnp.sqrt(lax.psum(jnp.sum(own * own), AXES))
    clip_norm = 0.5 * math.sqrt(2.0 * model_width * rank)
    factor = clip_norm / jnp.maximum(norm, clip_norm)
    return returns, own[:, :rank] * factor, own[:, rank:] * factor


def solution(mesh):
    placed = (
        P("batch", "seq", None),
        P("batch", "seq", None),
        P(),
        P(),
        P("batch", "seq"),
        P("batch", "seq"),
        P("batch", "seq"),
        P("batch"),
    )
    nb, ns = mesh.shape["batch"], mesh.shape["seq"]

    def step(hidden, *rest):
        powers = nb & (nb - 1) == 0 and ns & (ns - 1) == 0 and nb >= 2 and ns >= 8
        blocked = powers and hidden.shape[0] == nb and hidden.shape[2] == nb * ns * LANES
        return jax.shard_map(
            local_blocks if blocked else local_plain,
            mesh=mesh,
            in_specs=placed,
            out_specs=(P("batch", "seq"), P(AXES, None), P(AXES, None)),
            check_vma=False,
        )(hidden, *rest)

    return step
```

```python
import functools
import math

import jax
import jax.numpy as jnp
from jax import lax
from jax.experimental import pallas as pl
from jax.experimental.pallas import tpu as pltpu
from jax.sharding import PartitionSpec as P


ratio_cap = 2.0
weight_gain = 0.08
AXES = ("batch", "seq")
LANES = 128
KERNEL_VMEM = 8 * 1024 * 1024
F32 = jnp.float32

PARTS = (("yxzw", "xyzw", 16), ("xzwy", "yzwx", 14), ("zyxw", "zxyw", 19), ("xyzw", "yxzw", 15))
TURNS = (0, 1, 3, 2, 0, 1, 3, 2, 0, 2, 3, 1)

SMEM = pl.BlockSpec(memory_space=pltpu.SMEM)
VMEM = pl.BlockSpec(memory_space=pltpu.VMEM)
HBM = pl.BlockSpec(memory_space=pltpu.HBM)


def swap(x, mask, count):
    even, odd = mask if isinstance(mask, tuple) else (mask, mask)
    return lax.ppermute(x, AXES, [(i, i ^ (odd if i & 1 else even)) for i in range(count)])


class Line:
    def __init__(self):
        self.token = None
        self.placed = {}

    def place(self, x):
        x = pltpu.with_memory_space_constraint(x, pltpu.VMEM)
        self.placed[id(x)] = x
        return x

    def call(self, body, outs, ins, scalars=(), from_hbm=(), scratch=(), in_vmem=True, flops=0):
        first = self.token is None
        n_in = len(scalars) + len(from_hbm) + len(ins)

        def run(*refs):
            given, refs = refs[:n_in], refs[n_in:]
            if not first:
                refs = refs[1:]
            made, token, rest = refs[: len(outs)], refs[len(outs)], refs[len(outs) + 1 :]
            body(*given, *made, *rest)
            token[...] = jnp.zeros_like(token)

        kind = pltpu.VMEM if in_vmem else jax.ShapeDtypeStruct
        tokens = [] if first else [self.token]
        kernel = pl.pallas_call(
            run,
            out_shape=(*[kind(*o) for o in outs], pltpu.VMEM((8, LANES), F32)),
            in_specs=[SMEM] * len(scalars) + [HBM] * len(from_hbm) + [VMEM] * (len(ins) + len(tokens)),
            out_specs=(VMEM,) * (len(outs) + 1),
            scratch_shapes=list(scratch),
            compiler_params=pltpu.CompilerParams(vmem_limit_bytes=KERNEL_VMEM),
            cost_estimate=pl.CostEstimate(flops=flops, bytes_accessed=0, transcendentals=0) if flops else None,
        )
        from_hbm = [pltpu.with_memory_space_constraint(x, pltpu.HBM) for x in from_hbm]
        ins = [x if id(x) in self.placed else pltpu.with_memory_space_constraint(x, pltpu.VMEM) for x in [*ins, *tokens]]
        *got, self.token = kernel(*scalars, *from_hbm, *ins)
        return got


def row_of(tokens):
    return lax.broadcasted_iota(jnp.int32, (1, tokens), 1)


def first_body(length, rewards, live, group, *, total_len):
    tokens = rewards.shape[1]
    at = row_of(tokens)
    valid = jnp.where(at + lax.axis_index("seq") * tokens < length[0], 1.0, 0.0)
    row = rewards[...] * valid * jnp.exp(-at.astype(F32) / total_len)
    live[...] = row
    group[...] = jnp.broadcast_to(jnp.sum(row, axis=1, keepdims=True), group.shape)


def carry(group, other, carried, side, tokens, total_len):
    shard = lax.axis_index("seq")
    upper = jnp.full(group.shape, shard & side, jnp.int32) != 0
    steps = jnp.full(group.shape, side - 1 - (shard & (side - 1)), jnp.int32).astype(F32)
    here = jnp.where(upper, 0.0, jnp.exp(-steps * (tokens / total_len)))
    far = math.exp(-side * tokens / total_len)
    return jnp.where(upper, other + far * group, group + far * other), carried + here * other


def carry_body(group, other, carried, new_group, new_carried, **sizes):
    new_group[...], new_carried[...] = carry(group[...], other[...], carried[...], **sizes)


def project_body(src, mat, out_t, acc, *, steps):
    step = src.shape[1] // steps
    for i in range(steps):
        cut = slice(i * step, (i + 1) * step)
        part = jnp.dot(src[:, cut], mat[cut, :], preferred_element_type=F32)
        if i:
            part = part + acc[...]
        if i < steps - 1:
            acc[...] = part
        else:
            out_t[...] = part.T


def within_of(row, total_len):
    tokens = row.shape[1]
    first = row.astype(jnp.bfloat16)
    rest = row - first.astype(F32)
    second = rest.astype(jnp.bfloat16)
    third = (rest - second.astype(F32)).astype(jnp.bfloat16)
    rows = jnp.concatenate([first, second, third], axis=0)
    k_of = lax.broadcasted_iota(jnp.int32, (tokens, tokens), 0)
    t_of = lax.broadcasted_iota(jnp.int32, (tokens, tokens), 1)
    sums = jnp.dot(rows, (k_of >= t_of).astype(jnp.bfloat16), preferred_element_type=F32)
    return jnp.sum(sums, axis=0, keepdims=True) * jnp.exp(row_of(tokens).astype(F32) / total_len)


def within_body(row, within, *, total_len):
    within[...] = within_of(row[...], total_len)


def weigh_body(
    length, down_t, up_t, within, group, other, carried, values, log_ratio,
    returns, scaled_up, scaled_down, *, side, total_len, seq_total,
):
    rank, tokens = down_t.shape
    at = row_of(tokens)
    _, incoming = carry(group[...], other[...], carried[...], side, tokens, total_len)
    tail = jnp.exp((at - tokens).astype(F32) / total_len)
    back = within[...] + tail * incoming[0:1, 0:1]
    returns[...] = back
    adapter_scale = 1.0 / math.sqrt(rank)
    delta = adapter_scale * jnp.sum(down_t[...] * up_t[...], axis=0, keepdims=True)
    importance = jnp.exp(log_ratio[...] + delta)
    count = length[0]
    lens = jnp.full((1, tokens), count, jnp.int32).astype(F32)
    gain = weight_gain * math.sqrt(total_len * rank / seq_total) / lens
    valid = jnp.where(at + lax.axis_index("seq") * tokens < count, 1.0, 0.0)
    weight = -adapter_scale * (valid * jnp.minimum(importance, ratio_cap) * (back - values[...]) * gain)
    scaled_up[...] = (weight * up_t[...]).astype(jnp.bfloat16)
    scaled_down[...] = (weight * down_t[...]).astype(jnp.bfloat16)


def blocks_body(*refs, jobs, seq_size):
    hid, direction, scaled_up, scaled_down, *outs = refs
    me = lax.axis_index("batch") * seq_size + lax.axis_index("seq")
    odd = me & 1
    for out_at, tiles, row_at, rows, side, from_row in jobs:
        src, weight = ((hid, scaled_up), (direction, scaled_down))[side]
        out = outs[out_at]
        for i in range(0, len(tiles), 2):
            pair = tiles[i : i + 2]
            names = [even + odd * (other - even) for even, other in pair]
            cols = [src[:, pl.ds(pl.multiple_of((t ^ me) * LANES, LANES), LANES)] for t in names]
            block = jnp.concatenate(cols, axis=1) if len(cols) > 1 else cols[0]
            grad = jnp.dot(weight[from_row : from_row + rows, :], block, preferred_element_type=F32)
            for j in range(len(pair)):
                out[i + j, row_at : row_at + rows, :] = grad[:, j * LANES : (j + 1) * LANES]


def blocks(line, ops, wanted, seq_size):
    jobs, shapes = [], []
    for out_at, (tiles, pieces) in enumerate(wanted):
        at = 0
        for side, from_row, rows in pieces:
            jobs.append((out_at, tuple(tiles), at, rows, side, from_row))
            at += rows
        shapes.append(((len(tiles), at, LANES), F32))
    return line.call(functools.partial(blocks_body, jobs=tuple(jobs), seq_size=seq_size), shapes, ops)


def add_body(a, b, out):
    out[...] = a[...] + b[...]


def fold_body(*refs):
    *terms, send, left = refs
    half = send.shape[0]
    send[...] = functools.reduce(jnp.add, [t[half:] for t in terms])
    left[...] = functools.reduce(jnp.add, [t[:half] for t in terms])


def total_body(*refs, n, rank):
    keeps, gots, (down, up, squares) = refs[:n], refs[n : 2 * n], refs[2 * n :]
    at, row = 0, 0.0
    for keep, got in zip(keeps, gots):
        part = keep[0] + got[0]
        row = row + jnp.sum(part * part, axis=0, keepdims=True)
        rows = part.shape[0]
        split = min(max(rank - at, 0), rows)
        if split:
            down[at : at + split, :] = part[:split]
        if split < rows:
            up[at + split - rank : at + rows - rank, :] = part[split:]
        at += rows
    squares[...] = jnp.broadcast_to(row[None], squares.shape)


def clip_body(down, up, squares, grad_down, grad_up, *, clip_norm):
    norm = jnp.sqrt(jnp.sum(jnp.sum(squares[...], axis=0), axis=1, keepdims=True))
    factor = clip_norm / jnp.maximum(norm, clip_norm)
    grad_down[...] = (down[...] * factor).T
    grad_up[...] = (up[...] * factor).T


def tiles_of(order, fixed):
    names = [fixed]
    for mask in order:
        names = [n | b for n in names for b in (0, mask)]
    return names


def log2(n):
    return n.bit_length() - 1


def script(halvings):
    n = len(PARTS)
    first = list(range(n))
    steps = [("blocks", 0, 0)]
    for i in first:
        steps += [("blocks", i + 1, 0), ("add", i, 0)]
    steps += [("far_rest", 0, 0), ("near_rest", 0, 0)]
    turns = TURNS if len(TURNS) == n * (halvings - 1) else first * (halvings - 1)
    taken = [1] * n
    for i in turns:
        steps.append(("fold", i, taken[i]))
        taken[i] += 1
    return steps


def local_blocks(hidden, score_direction, adapter_down, adapter_up, rewards, values, log_ratio, lengths):
    return in_blocks(hidden, score_direction, adapter_down, adapter_up, rewards, values, log_ratio, lengths)


def in_blocks(hidden, score_direction, adapter_down, adapter_up, rewards, values, log_ratio, lengths):
    _, tokens, width = hidden.shape
    rank = adapter_down.shape[1]
    nb, ns = lax.axis_size("batch"), lax.axis_size("seq")
    count = nb * ns
    total_len = tokens * ns
    hid_hbm, direction_hbm = hidden[0], score_direction[0]
    line = Line()

    bits = [1 << j for j in range(log2(ns))]
    tile = ((8, LANES), F32)
    FL = 40_000_000_000
    live, group = line.call(
        functools.partial(first_body, total_len=total_len), [((1, tokens), F32), tile], (rewards,), (lengths,)
    )
    carried = jnp.zeros(*tile)
    hid, direction = line.place(hid_hbm), line.place(direction_hbm)
    under = [(hid, adapter_down), (direction, adapter_up)]
    made = []
    for j, side in enumerate(bits):
        other = swap(group, side, count)
        if j == 0:
            (within,) = line.call(functools.partial(within_body, total_len=total_len), [((1, tokens), F32)], (live,), flops=FL)
        if j >= len(bits) - len(under):
            (proj,) = line.call(
                functools.partial(project_body, steps=2),
                [((rank, tokens), F32)],
                under[len(made)],
                scratch=[pltpu.VMEM((tokens, rank), F32)],
            )
            made.append(proj)
        if j < len(bits) - 1:
            group, carried = line.call(
                functools.partial(carry_body, side=side, tokens=tokens, total_len=total_len),
                [tile, tile], (group, other, carried),
            )
    down_t, up_t = made
    returns, scaled_up, scaled_down = line.call(
        functools.partial(weigh_body, side=bits[-1], total_len=total_len, seq_total=nb),
        [((1, tokens), F32), ((rank, tokens), jnp.bfloat16), ((rank, tokens), jnp.bfloat16)],
        (down_t, up_t, within, group, other, carried, values, log_ratio), (lengths,),
    )

    ops = (hid, direction, scaled_up, scaled_down)
    core, plane = bits[0], bits[1:]
    zs = [ns << j for j in range(log2(nb))]
    masks = {"x": plane[: len(plane) // 2], "y": plane[len(plane) // 2 :], "z": zs[:-1], "w": zs[-1:]}
    orders, pieces, at = [], [], 0
    for even, odd, share in PARTS:
        orders.append([[m for axis in axes for m in masks[axis]] for axes in (even, odd)])
        end = at + 2 * rank * share // 64
        pieces.append([
            (side, max(at - side * rank, 0), min(end, rank * (side + 1)) - max(at, rank * side))
            for side in (0, 1)
            if min(end, rank * (side + 1)) > max(at, rank * side)
        ])
        at = end
    n = len(PARTS)
    sends = [(list(zip(*[tiles_of(o[1:], o[0]) for o in orders[i]])), pieces[i]) for i in range(n)]
    stays = [(list(zip(*[tiles_of(o[1:], 0) for o in orders[i]])), pieces[i]) for i in range(n)]
    far = lambda w: ([(odd | core, even | core) for even, odd in w[0]], w[1])
    got, near, sent, kept = [None] * n, [None] * n, [None] * n, [None] * n
    for name, i, k in script(len(orders[0][0])):
        if name == "blocks":
            want = ([sends[i - 1]] if i else []) + ([far(sends[i])] if i < n else [])
            made = list(blocks(line, ops, want, ns))
            if i:
                near[i - 1] = made.pop(0)
            if i < n:
                got[i] = swap(made[0], core, count)
        elif name == "far_rest":
            rest = [swap(t, core, count) for t in blocks(line, ops, [far(w) for w in stays], ns)]
        elif name == "near_rest":
            kept = [(a, b) for a, b in zip(blocks(line, ops, stays, ns), rest)]
        else:
            if name == "add":
                (send,) = line.call(add_body, [(near[i].shape, F32)], (near[i], got[i]))
            else:
                terms = (*kept[i], sent[i])
                blocks_now, rows, _ = terms[0].shape
                send, left = line.call(fold_body, [((blocks_now // 2, rows, LANES), F32)] * 2, terms)
                kept[i] = (left,)
            sent[i] = swap(send, tuple(o[k] for o in orders[i]), count)

    down, up, squares = line.call(
        functools.partial(total_body, n=n, rank=rank),
        [((rank, LANES), F32), ((rank, LANES), F32), ((count, 1, LANES), F32)], (*[k[0] for k in kept], *sent),
    )
    squares = lax.all_to_all(squares, AXES, 0, 0, tiled=True)
    clip_norm = 0.5 * math.sqrt(2.0 * width * rank)
    grad_down, grad_up = line.call(
        functools.partial(clip_body, clip_norm=clip_norm), [((LANES, rank), F32)] * 2, (down, up, squares), in_vmem=False
    )
    return returns, grad_down, grad_up


def local_plain(hidden, score_direction, adapter_down, adapter_up, rewards, values, log_ratio, lengths):
    seq_count, shard_len, model_width = hidden.shape
    rank = adapter_down.shape[1]
    ns = lax.axis_size("seq")
    total_len = shard_len * ns
    seq_total = seq_count * lax.axis_size("batch")
    shard = lax.axis_index("seq")
    inner = jnp.arange(shard_len, dtype=jnp.int32)
    valid = ((shard * shard_len + inner)[None, :] < lengths[:, None]).astype(F32)
    scale = 1.0 / math.sqrt(rank)
    down = jnp.einsum("ogz,zw->ogw", hidden, adapter_down, preferred_element_type=F32)
    up = jnp.einsum("ogz,zw->ogw", score_direction, adapter_up, preferred_element_type=F32)
    importance = jnp.exp(log_ratio + scale * jnp.sum(down * up, axis=-1))
    live = rewards * valid
    offsets = (inner[None, :] - inner[:, None]).astype(F32)
    discount = jnp.where(offsets >= 0, jnp.exp(-offsets / total_len), jnp.zeros_like(offsets))
    within = jnp.einsum("sk,tk->st", live, discount, precision=lax.Precision.HIGHEST)
    firsts = lax.all_gather(within[:, :1], "seq", axis=1, tiled=True)
    index = jnp.arange(ns, dtype=jnp.int32)
    steps = (index - shard - 1).astype(F32)
    here = jnp.where(index > shard, jnp.exp(-steps * shard_len / total_len), jnp.zeros_like(steps))
    carried = jnp.sum(firsts * here[None, :], axis=1)
    tail = jnp.exp(-(shard_len - inner).astype(F32) / total_len)
    returns = within + tail[None, :] * carried[:, None]
    gain = weight_gain * math.sqrt(total_len * rank / seq_total) / lengths.astype(F32)
    weight = valid * jnp.minimum(importance, ratio_cap) * (returns - values) * gain[:, None]
    scaled_up = (-scale * weight[:, :, None] * up).astype(jnp.bfloat16)
    scaled_down = (-scale * weight[:, :, None] * down).astype(jnp.bfloat16)
    terms = jnp.concatenate(
        [
            jnp.einsum("oxe,oxq->eq", hidden, scaled_up, preferred_element_type=F32),
            jnp.einsum("oxe,oxq->eq", score_direction, scaled_down, preferred_element_type=F32),
        ],
        axis=1,
    )
    own = lax.psum_scatter(terms, AXES, scatter_dimension=0, tiled=True)
    norm = jnp.sqrt(lax.psum(jnp.sum(own * own), AXES))
    clip_norm = 0.5 * math.sqrt(2.0 * model_width * rank)
    factor = clip_norm / jnp.maximum(norm, clip_norm)
    return returns, own[:, :rank] * factor, own[:, rank:] * factor


def solution(mesh):
    placed = (
        P("batch", "seq", None),
        P("batch", "seq", None),
        P(),
        P(),
        P("batch", "seq"),
        P("batch", "seq"),
        P("batch", "seq"),
        P("batch"),
    )
    nb, ns = mesh.shape["batch"], mesh.shape["seq"]

    def step(hidden, *rest):
        powers = nb & (nb - 1) == 0 and ns & (ns - 1) == 0 and nb >= 2 and ns >= 8
        blocked = powers and hidden.shape[0] == nb and hidden.shape[2] == nb * ns * LANES
        return jax.shard_map(
            local_blocks if blocked else local_plain,
            mesh=mesh,
            in_specs=placed,
            out_specs=(P("batch", "seq"), P(AXES, None), P(AXES, None)),
            check_vma=False,
        )(hidden, *rest)

    return step
```

```python
import functools
import itertools
import math

import jax
import jax.numpy as jnp
from jax import lax
from jax.experimental import pallas as pl
from jax.experimental.pallas import tpu as pltpu
from jax.sharding import PartitionSpec as P


ratio_cap = 2.0
weight_gain = 0.08
AXES = ("batch", "seq")
LANES = 128
KERNEL_VMEM = 8 * 1024 * 1024
F32 = jnp.float32

PARTS = (("yxzw", "xyzw", 17), ("xzwy", "yzwx", 13), ("zyxw", "zxyw", 19), ("xyzw", "yxzw", 15))
TURNS = (0, 1, 3, 2, 0, 1, 3, 2, 0, 2, 3, 1)

SMEM = pl.BlockSpec(memory_space=pltpu.SMEM)
VMEM = pl.BlockSpec(memory_space=pltpu.VMEM)
HBM = pl.BlockSpec(memory_space=pltpu.HBM)


def swap(x, mask, count):
    even, odd = mask if isinstance(mask, tuple) else (mask, mask)
    return lax.ppermute(x, AXES, [(i, i ^ (odd if i & 1 else even)) for i in range(count)])


class Line:
    def __init__(self):
        self.token = None
        self.placed = {}

    def place(self, x):
        x = pltpu.with_memory_space_constraint(x, pltpu.VMEM)
        self.placed[id(x)] = x
        return x

    def call(self, body, outs, ins, scalars=(), from_hbm=(), scratch=(), in_vmem=True, flops=0):
        first = self.token is None
        n_in = len(scalars) + len(from_hbm) + len(ins)

        def run(*refs):
            given, refs = refs[:n_in], refs[n_in:]
            if not first:
                refs = refs[1:]
            made, token, rest = refs[: len(outs)], refs[len(outs)], refs[len(outs) + 1 :]
            body(*given, *made, *rest)
            token[...] = jnp.zeros_like(token)

        kind = pltpu.VMEM if in_vmem else jax.ShapeDtypeStruct
        tokens = [] if first else [self.token]
        kernel = pl.pallas_call(
            run,
            out_shape=(*[kind(*o) for o in outs], pltpu.VMEM((8, LANES), F32)),
            in_specs=[SMEM] * len(scalars) + [HBM] * len(from_hbm) + [VMEM] * (len(ins) + len(tokens)),
            out_specs=(VMEM,) * (len(outs) + 1),
            scratch_shapes=list(scratch),
            compiler_params=pltpu.CompilerParams(vmem_limit_bytes=KERNEL_VMEM),
            cost_estimate=pl.CostEstimate(flops=flops, bytes_accessed=0, transcendentals=0) if flops else None,
        )
        from_hbm = [pltpu.with_memory_space_constraint(x, pltpu.HBM) for x in from_hbm]
        ins = [x if id(x) in self.placed else pltpu.with_memory_space_constraint(x, pltpu.VMEM) for x in [*ins, *tokens]]
        *got, self.token = kernel(*scalars, *from_hbm, *ins)
        return got


def row_of(tokens):
    return lax.broadcasted_iota(jnp.int32, (1, tokens), 1)


def first_body(length, rewards, live, group, *, total_len):
    tokens = rewards.shape[1]
    at = row_of(tokens)
    valid = jnp.where(at + lax.axis_index("seq") * tokens < length[0], 1.0, 0.0)
    row = rewards[...] * valid * jnp.exp(-at.astype(F32) / total_len)
    live[...] = row
    group[...] = jnp.broadcast_to(jnp.sum(row, axis=1, keepdims=True), group.shape)


def carry(group, other, carried, side, tokens, total_len):
    shard = lax.axis_index("seq")
    upper = jnp.full(group.shape, shard & side, jnp.int32) != 0
    steps = jnp.full(group.shape, side - 1 - (shard & (side - 1)), jnp.int32).astype(F32)
    here = jnp.where(upper, 0.0, jnp.exp(-steps * (tokens / total_len)))
    far = math.exp(-side * tokens / total_len)
    return jnp.where(upper, other + far * group, group + far * other), carried + here * other


def carry_body(group, other, carried, new_group, new_carried, **sizes):
    new_group[...], new_carried[...] = carry(group[...], other[...], carried[...], **sizes)


def project_body(src, mat, out_t, acc, *, steps):
    step = src.shape[1] // steps
    for i in range(steps):
        cut = slice(i * step, (i + 1) * step)
        part = jnp.dot(src[:, cut], mat[cut, :], preferred_element_type=F32)
        if i:
            part = part + acc[...]
        if i < steps - 1:
            acc[...] = part
        else:
            out_t[...] = part.T


def within_of(row, total_len):
    tokens = row.shape[1]
    first = row.astype(jnp.bfloat16)
    rest = row - first.astype(F32)
    second = rest.astype(jnp.bfloat16)
    third = (rest - second.astype(F32)).astype(jnp.bfloat16)
    rows = jnp.concatenate([first, second, third], axis=0)
    k_of = lax.broadcasted_iota(jnp.int32, (tokens, tokens), 0)
    t_of = lax.broadcasted_iota(jnp.int32, (tokens, tokens), 1)
    sums = jnp.dot(rows, (k_of >= t_of).astype(jnp.bfloat16), preferred_element_type=F32)
    return jnp.sum(sums, axis=0, keepdims=True) * jnp.exp(row_of(tokens).astype(F32) / total_len)


def within_body(row, within, *, total_len):
    within[...] = within_of(row[...], total_len)


def weigh_body(
    length, down_t, up_t, within, group, other, carried, values, log_ratio,
    returns, scaled_up, scaled_down, *, side, total_len, seq_total,
):
    rank, tokens = down_t.shape
    at = row_of(tokens)
    _, incoming = carry(group[...], other[...], carried[...], side, tokens, total_len)
    tail = jnp.exp((at - tokens).astype(F32) / total_len)
    back = within[...] + tail * incoming[0:1, 0:1]
    returns[...] = back
    adapter_scale = 1.0 / math.sqrt(rank)
    delta = adapter_scale * jnp.sum(down_t[...] * up_t[...], axis=0, keepdims=True)
    importance = jnp.exp(log_ratio[...] + delta)
    count = length[0]
    lens = jnp.full((1, tokens), count, jnp.int32).astype(F32)
    gain = weight_gain * math.sqrt(total_len * rank / seq_total) / lens
    valid = jnp.where(at + lax.axis_index("seq") * tokens < count, 1.0, 0.0)
    weight = -adapter_scale * (valid * jnp.minimum(importance, ratio_cap) * (back - values[...]) * gain)
    scaled_up[...] = (weight * up_t[...]).astype(jnp.bfloat16)
    scaled_down[...] = (weight * down_t[...]).astype(jnp.bfloat16)


def blocks_body(*refs, jobs, seq_size):
    hid, direction, scaled_up, scaled_down, *outs = refs
    me = lax.axis_index("batch") * seq_size + lax.axis_index("seq")
    odd = me & 1
    for out_at, tiles, row_at, rows, side, from_row in jobs:
        src, weight = ((hid, scaled_up), (direction, scaled_down))[side]
        out = outs[out_at]
        for i in range(0, len(tiles), 2):
            pair = tiles[i : i + 2]
            names = [even + odd * (other - even) for even, other in pair]
            cols = [src[:, pl.ds(pl.multiple_of((t ^ me) * LANES, LANES), LANES)] for t in names]
            block = jnp.concatenate(cols, axis=1) if len(cols) > 1 else cols[0]
            grad = jnp.dot(weight[from_row : from_row + rows, :], block, preferred_element_type=F32)
            for j in range(len(pair)):
                out[i + j, row_at : row_at + rows, :] = grad[:, j * LANES : (j + 1) * LANES]


def blocks(line, ops, wanted, seq_size):
    jobs, shapes = [], []
    for out_at, (tiles, pieces) in enumerate(wanted):
        at = 0
        for side, from_row, rows in pieces:
            jobs.append((out_at, tuple(tiles), at, rows, side, from_row))
            at += rows
        shapes.append(((len(tiles), at, LANES), F32))
    return line.call(functools.partial(blocks_body, jobs=tuple(jobs), seq_size=seq_size), shapes, ops)


def add_body(a, b, out):
    out[...] = a[...] + b[...]


def fold_body(*refs):
    *terms, send, left = refs
    half = send.shape[0]
    send[...] = functools.reduce(jnp.add, [t[half:] for t in terms])
    left[...] = functools.reduce(jnp.add, [t[:half] for t in terms])


def total_body(*refs, n, rank):
    keeps, gots, (down, up, squares) = refs[:n], refs[n : 2 * n], refs[2 * n :]
    at, row = 0, 0.0
    for keep, got in zip(keeps, gots):
        part = keep[0] + got[0]
        row = row + jnp.sum(part * part, axis=0, keepdims=True)
        rows = part.shape[0]
        split = min(max(rank - at, 0), rows)
        if split:
            down[at : at + split, :] = part[:split]
        if split < rows:
            up[at + split - rank : at + rows - rank, :] = part[split:]
        at += rows
    squares[...] = jnp.broadcast_to(row[None], squares.shape)


def clip_body(down, up, squares, grad_down, grad_up, *, clip_norm):
    norm = jnp.sqrt(jnp.sum(jnp.sum(squares[...], axis=0), axis=1, keepdims=True))
    factor = clip_norm / jnp.maximum(norm, clip_norm)
    grad_down[...] = down[...] * factor
    grad_up[...] = up[...] * factor


def turn_body(down, up, down_rows, up_rows):
    down_rows[...] = down[...].T
    up_rows[...] = up[...].T


def tiles_of(order, fixed):
    names = [fixed]
    for mask in order:
        names = [n | b for n in names for b in (0, mask)]
    return names


def log2(n):
    return n.bit_length() - 1


def laying():
    n = len(PARTS)
    for size in range(1, n):
        for some in itertools.combinations(range(n), size):
            if sum(PARTS[i][2] for i in some) == 32:
                return [*some, *[i for i in range(n) if i not in some]]
    return list(range(n))


def script(halvings):
    n = len(PARTS)
    first = list(range(n))
    steps = [("blocks", 0, 0)]
    for i in first:
        steps += [("blocks", i + 1, 0), ("add", i, 0)]
    steps += [("far_rest", 0, 0), ("near_rest", 0, 0)]
    turns = TURNS if len(TURNS) == n * (halvings - 1) else first * (halvings - 1)
    taken = [1] * n
    for i in turns:
        steps.append(("fold", i, taken[i]))
        taken[i] += 1
    return steps


def local_blocks(hidden, score_direction, adapter_down, adapter_up, rewards, values, log_ratio, lengths):
    return in_blocks(hidden, score_direction, adapter_down, adapter_up, rewards, values, log_ratio, lengths)


def in_blocks(hidden, score_direction, adapter_down, adapter_up, rewards, values, log_ratio, lengths):
    _, tokens, width = hidden.shape
    rank = adapter_down.shape[1]
    nb, ns = lax.axis_size("batch"), lax.axis_size("seq")
    count = nb * ns
    total_len = tokens * ns
    hid_hbm, direction_hbm = hidden[0], score_direction[0]
    line = Line()

    bits = [1 << j for j in range(log2(ns))]
    tile = ((8, LANES), F32)
    FL = 40_000_000_000
    live, group = line.call(
        functools.partial(first_body, total_len=total_len), [((1, tokens), F32), tile], (rewards,), (lengths,)
    )
    carried = jnp.zeros(*tile)
    hid, direction = line.place(hid_hbm), line.place(direction_hbm)
    under = [(hid, adapter_down), (direction, adapter_up)]
    made = []
    for j, side in enumerate(bits):
        other = swap(group, side, count)
        if j == 0:
            (within,) = line.call(functools.partial(within_body, total_len=total_len), [((1, tokens), F32)], (live,), flops=FL)
        if j >= len(bits) - len(under):
            (proj,) = line.call(
                functools.partial(project_body, steps=2),
                [((rank, tokens), F32)],
                under[len(made)],
                scratch=[pltpu.VMEM((tokens, rank), F32)],
            )
            made.append(proj)
        if j < len(bits) - 1:
            group, carried = line.call(
                functools.partial(carry_body, side=side, tokens=tokens, total_len=total_len),
                [tile, tile], (group, other, carried),
            )
    down_t, up_t = made
    returns, scaled_up, scaled_down = line.call(
        functools.partial(weigh_body, side=bits[-1], total_len=total_len, seq_total=nb),
        [((1, tokens), F32), ((rank, tokens), jnp.bfloat16), ((rank, tokens), jnp.bfloat16)],
        (down_t, up_t, within, group, other, carried, values, log_ratio), (lengths,),
    )

    ops = (hid, direction, scaled_up, scaled_down)
    core, plane = bits[0], bits[1:]
    zs = [ns << j for j in range(log2(nb))]
    masks = {"x": plane[: len(plane) // 2], "y": plane[len(plane) // 2 :], "z": zs[:-1], "w": zs[-1:]}
    orders = [[[m for axis in axes for m in masks[axis]] for axes in part[:2]] for part in PARTS]
    pieces, at, laid = [None] * len(PARTS), 0, laying()
    for i in laid:
        end = at + 2 * rank * PARTS[i][2] // 64
        pieces[i] = [
            (side, max(at - side * rank, 0), min(end, rank * (side + 1)) - max(at, rank * side))
            for side in (0, 1)
            if min(end, rank * (side + 1)) > max(at, rank * side)
        ]
        at = end
    n = len(PARTS)
    sends = [(list(zip(*[tiles_of(o[1:], o[0]) for o in orders[i]])), pieces[i]) for i in range(n)]
    stays = [(list(zip(*[tiles_of(o[1:], 0) for o in orders[i]])), pieces[i]) for i in range(n)]
    far = lambda w: ([(odd | core, even | core) for even, odd in w[0]], w[1])
    got, near, sent, kept = [None] * n, [None] * n, [None] * n, [None] * n
    for name, i, k in script(len(orders[0][0])):
        if name == "blocks":
            want = ([sends[i - 1]] if i else []) + ([far(sends[i])] if i < n else [])
            made = list(blocks(line, ops, want, ns))
            if i:
                near[i - 1] = made.pop(0)
            if i < n:
                got[i] = swap(made[0], core, count)
        elif name == "far_rest":
            rest = [swap(t, core, count) for t in blocks(line, ops, [far(w) for w in stays], ns)]
        elif name == "near_rest":
            kept = [(a, b) for a, b in zip(blocks(line, ops, stays, ns), rest)]
        else:
            if name == "add":
                (send,) = line.call(add_body, [(near[i].shape, F32)], (near[i], got[i]))
            else:
                terms = (*kept[i], sent[i])
                blocks_now, rows, _ = terms[0].shape
                send, left = line.call(fold_body, [((blocks_now // 2, rows, LANES), F32)] * 2, terms)
                kept[i] = (left,)
            sent[i] = swap(send, tuple(o[k] for o in orders[i]), count)

    down, up, squares = line.call(
        functools.partial(total_body, n=n, rank=rank),
        [((rank, LANES), F32), ((rank, LANES), F32), ((count, 1, LANES), F32)], (*[kept[i][0] for i in laid], *[sent[i] for i in laid]),
    )
    squares = lax.all_to_all(squares, AXES, 0, 0, tiled=True)
    down, up = line.call(turn_body, [((LANES, rank), F32)] * 2, (down, up))
    clip_norm = 0.5 * math.sqrt(2.0 * width * rank)
    grad_down, grad_up = line.call(
        functools.partial(clip_body, clip_norm=clip_norm), [((LANES, rank), F32)] * 2, (down, up, squares), in_vmem=False
    )
    return returns, grad_down, grad_up


def local_plain(hidden, score_direction, adapter_down, adapter_up, rewards, values, log_ratio, lengths):
    seq_count, shard_len, model_width = hidden.shape
    rank = adapter_down.shape[1]
    ns = lax.axis_size("seq")
    total_len = shard_len * ns
    seq_total = seq_count * lax.axis_size("batch")
    shard = lax.axis_index("seq")
    inner = jnp.arange(shard_len, dtype=jnp.int32)
    valid = ((shard * shard_len + inner)[None, :] < lengths[:, None]).astype(F32)
    scale = 1.0 / math.sqrt(rank)
    down = jnp.einsum("ogz,zw->ogw", hidden, adapter_down, preferred_element_type=F32)
    up = jnp.einsum("ogz,zw->ogw", score_direction, adapter_up, preferred_element_type=F32)
    importance = jnp.exp(log_ratio + scale * jnp.sum(down * up, axis=-1))
    live = rewards * valid
    offsets = (inner[None, :] - inner[:, None]).astype(F32)
    discount = jnp.where(offsets >= 0, jnp.exp(-offsets / total_len), jnp.zeros_like(offsets))
    within = jnp.einsum("sk,tk->st", live, discount, precision=lax.Precision.HIGHEST)
    firsts = lax.all_gather(within[:, :1], "seq", axis=1, tiled=True)
    index = jnp.arange(ns, dtype=jnp.int32)
    steps = (index - shard - 1).astype(F32)
    here = jnp.where(index > shard, jnp.exp(-steps * shard_len / total_len), jnp.zeros_like(steps))
    carried = jnp.sum(firsts * here[None, :], axis=1)
    tail = jnp.exp(-(shard_len - inner).astype(F32) / total_len)
    returns = within + tail[None, :] * carried[:, None]
    gain = weight_gain * math.sqrt(total_len * rank / seq_total) / lengths.astype(F32)
    weight = valid * jnp.minimum(importance, ratio_cap) * (returns - values) * gain[:, None]
    scaled_up = (-scale * weight[:, :, None] * up).astype(jnp.bfloat16)
    scaled_down = (-scale * weight[:, :, None] * down).astype(jnp.bfloat16)
    terms = jnp.concatenate(
        [
            jnp.einsum("oxe,oxq->eq", hidden, scaled_up, preferred_element_type=F32),
            jnp.einsum("oxe,oxq->eq", score_direction, scaled_down, preferred_element_type=F32),
        ],
        axis=1,
    )
    own = lax.psum_scatter(terms, AXES, scatter_dimension=0, tiled=True)
    norm = jnp.sqrt(lax.psum(jnp.sum(own * own), AXES))
    clip_norm = 0.5 * math.sqrt(2.0 * model_width * rank)
    factor = clip_norm / jnp.maximum(norm, clip_norm)
    return returns, own[:, :rank] * factor, own[:, rank:] * factor


def solution(mesh):
    placed = (
        P("batch", "seq", None),
        P("batch", "seq", None),
        P(),
        P(),
        P("batch", "seq"),
        P("batch", "seq"),
        P("batch", "seq"),
        P("batch"),
    )
    nb, ns = mesh.shape["batch"], mesh.shape["seq"]

    def step(hidden, *rest):
        powers = nb & (nb - 1) == 0 and ns & (ns - 1) == 0 and nb >= 2 and ns >= 8
        blocked = powers and hidden.shape[0] == nb and hidden.shape[2] == nb * ns * LANES
        return jax.shard_map(
            local_blocks if blocked else local_plain,
            mesh=mesh,
            in_specs=placed,
            out_specs=(P("batch", "seq"), P(AXES, None), P(AXES, None)),
            check_vma=False,
        )(hidden, *rest)

    return step
```
